32 devices in a mesh: dp: 2 (over z, core), ep: 16 (over x, y).
Axes of the slice: x: 4, y: 4, z: 1, core: 2. Of those that a mesh axis runs over, the one named last changes fastest.
The devices are a block of a 4x4x8 slice.
Arguments:
- x: bfloat16 [2, 16, 256, 1792], P('dp', 'ep'), parts along dimension 0
- expert: int32 [2, 16, 256, 2], P('dp', 'ep'), parts along dimension 0
- slot: int32 [2, 16, 256, 2], P('dp', 'ep'), parts along dimension 0
- gate: float32 [2, 16, 256, 2], P('dp', 'ep'), parts along dimension 0
- w_gate: bfloat16 [32, 1792, 4864], P('ep')
- w_up: bfloat16 [32, 1792, 4864], P('ep')
- w_down: bfloat16 [32, 4864, 1792], P('ep')
Outputs:
- y: bfloat16 [2, 16, 256, 1792], P('dp', 'ep'), parts along dimension 0
There are 2 independent parts. The reference program is written for one: setup_inputs(seed, part) draws one part's arguments, and reference() takes and returns one part's arrays. A program takes and returns all parts, laid end to end along the dimension named above; an argument that names none is the same for every part.
All inputs are finite; a program needn't handle non-finite values.
Results may differ from the reference program's by a relative error of at most 0.009.
Values are sent between devices in bfloat16 or wider.
A program may use at most 768 MiB of HBM per device.

```python
import jax
import jax.numpy as jnp

MEMBERS = 16
TOKENS = 256
D = 1792
FF = 4864
TOP = 2
EXPERTS = 32
SLOTS = 5 * TOKENS * TOP // (4 * EXPERTS)


def setup_inputs(seed: int = 0, part: int = 0) -> dict:
    own, k1, k2, k3, k4, k5, k6 = jax.random.split(jax.random.key(seed), 7)
    kx, ke, kl, kg = jax.random.split(jax.random.fold_in(own, part), 4)
    devices = (1, MEMBERS)
    place = jax.random.permutation(kl, jnp.arange(EXPERTS, dtype=jnp.uint32))
    slow = ((EXPERTS + (9 * place) % EXPERTS) << ((9 * place) // EXPERTS)) // EXPERTS
    wait = (jax.random.bits(ke, (*devices, TOKENS, EXPERTS), jnp.uint32) >> 10) * slow
    expert = jnp.argsort(wait, axis=-1)[..., :TOP].astype(jnp.int32)
    chosen = jax.nn.one_hot(expert, EXPERTS, dtype=jnp.int32)
    in_line = jnp.cumsum(chosen.reshape(*devices, TOKENS * TOP, EXPERTS), axis=2) - 1
    slot = jnp.sum(in_line.reshape(chosen.shape) * chosen, axis=-1)

    def one(key, rows, columns):
        return (jax.random.normal(key, (rows, columns), jnp.float32) * rows**-0.5).astype(jnp.bfloat16)

    def weights(key, rows, columns):
        return jax.lax.map(lambda k: one(k, rows, columns), jax.random.split(key, EXPERTS))

    return {
        "x": jax.random.normal(kx, (*devices, TOKENS, D), jnp.float32).astype(jnp.bfloat16),
        "expert": expert,
        "slot": slot,
        "gate": jax.nn.softmax(jax.random.normal(kg, expert.shape, jnp.float32)),
        "w_gate": weights(k1, D, FF),
        "w_up": weights(k2, D, FF),
        "w_down": weights(k3, FF, D),
    }


def einsum(form, a, b):
    return jnp.einsum(form, a.astype(jnp.float32), b.astype(jnp.float32))


def reference(x, expert, slot, gate, w_gate, w_up, w_down):
    to_expert = jax.nn.one_hot(expert, EXPERTS, dtype=jnp.bfloat16)
    to_slot = jax.nn.one_hot(slot, SLOTS, dtype=jnp.bfloat16)
    weighted = to_expert * gate[..., None].astype(jnp.bfloat16)
    dispatch = einsum("abtke,abtkc->abtec", to_expert, to_slot).astype(jnp.bfloat16)
    combine = einsum("abtke,abtkc->abtec", weighted, to_slot).astype(jnp.bfloat16)
    z = einsum("abtec,abtd->aebcd", dispatch, x).astype(jnp.bfloat16)
    h = jax.nn.silu(einsum("aebcd,edf->aebcf", z, w_gate))
    h = (h * einsum("aebcd,edf->aebcf", z, w_up)).astype(jnp.bfloat16)
    out = einsum("aebcf,efd->aebcd", h, w_down).astype(jnp.bfloat16)
    y = einsum("abtec,aebcd->abtd", combine, out)
    return y.astype(jnp.bfloat16)
```

```python
import functools

import jax
import jax.numpy as jnp
from jax import lax
from jax.experimental import pallas as pl
from jax.experimental.pallas import tpu as pltpu
from jax.sharding import PartitionSpec as P

MESH = pl.DeviceIdType.MESH
FT = 256
NT = 512
ROWS = 16
UNROLL = 3


def dot(a, b):
    return jnp.dot(a, b, preferred_element_type=jnp.float32)


def kernel(
    side, slots,
    x_hbm, expert_ref, slot_ref, gate_ref, wg, wu, wd, y_hbm,
    xs, gu, dn, h, zc, snd, snd_c, rcv, rcv_c, ret, ret_c,
    sem_x, sem_g, sem_d, sem_ds, sem_dr, sem_cs, sem_cr, sem_y,
):
    members = side * side
    tokens, width = xs.shape
    hidden = h.shape[1]
    steps = hidden // FT
    rest = slots - ROWS
    dp, ep = lax.axis_index("dp"), lax.axis_index("ep")
    core = lax.rem(dp, 2)
    base = dp - core
    px, py = ep // side, lax.rem(ep, side)
    tiles = [(n, min(NT, width - n)) for n in range(0, width, NT)]
    blocks = members

    def place(i, chunk):
        dx = i // (2 * side)
        return (dx if chunk == 2 else 2 * dx + chunk), (i // 2) % side

    def ahead(i, chunk):
        dx, dy = place(i, chunk)
        return ((px + dx) % side) * side + (py + dy) % side

    def behind(i, chunk):
        dx, dy = place(i, chunk)
        return ((px + side - dx) % side) * side + (py + side - dy) % side

    def others(chunk):
        return {0: blocks - 1, 1: blocks, 2: 2 * blocks - 1}[chunk]

    def block_of(i, chunk):
        if chunk == 1:
            return i
        i = i + 1
        return i // 2 * 2 + (i + core) % 2

    copy_x = pltpu.make_async_copy(x_hbm.at[0, 0], xs, sem_x)
    copy_x.start()

    barrier = pltpu.get_barrier_semaphore()

    def greet(i, c):
        j = block_of(i, 2)
        pl.semaphore_signal(
            barrier, inc=1, device_id=(base + j % 2, ahead(j, 2)), device_id_type=MESH
        )
        return c

    lax.fori_loop(0, others(2), greet, 0)

    def gu_copies(s):
        cols = pl.ds(pl.multiple_of(s * FT, FT), FT)
        return (
            pltpu.make_async_copy(wg.at[core, :, cols], gu.at[s, :, pl.ds(0, FT)], sem_g.at[s, 0]),
            pltpu.make_async_copy(wu.at[core, :, cols], gu.at[s, :, pl.ds(FT, FT)], sem_g.at[s, 1]),
        )

    def dn_copy(t):
        n, size = tiles[t]
        return pltpu.make_async_copy(wd.at[core, :, pl.ds(n, size)], dn.at[:, pl.ds(n, size)], sem_d.at[t])

    copy_x.wait()

    def start_gu(s, c):
        for copy in gu_copies(s):
            copy.start()
        return c

    lax.fori_loop(0, steps, start_gu, 0)
    for t in range(len(tiles)):
        dn_copy(t).start()

    slot, expert = slot_ref[0, 0], expert_ref[0, 0]
    code = jnp.where(slot < slots, expert * slots + slot, -1)
    down0, down1 = code[:, 0:1], code[:, 1:2]
    across0 = jnp.transpose(jnp.broadcast_to(down0, (tokens, 128)))[0:1]
    across1 = jnp.transpose(jnp.broadcast_to(down1, (tokens, 128)))[0:1]
    gates = gate_ref[0, 0].astype(jnp.bfloat16).astype(jnp.float32)

    def row_code(row, chunk):
        i, j = row // 16, row % 16
        if chunk == 2:
            return (2 * ahead(i, 2) + i % 2) * slots + ROWS + j % 4, j // 4
        return (2 * ahead(i, chunk) + i % 2) * slots + j, None

    def gather_mask(chunk, rows):
        row = lax.broadcasted_iota(jnp.int32, (rows, tokens), 0)
        code, quarter = row_code(row, chunk)
        hit = (code == across0) | (code == across1)
        if chunk == 2:
            hit = hit & (row % 4 < rest)
        return hit, quarter

    def ones(mask):
        return jnp.where(mask, 1.0, 0.0).astype(jnp.bfloat16)

    def send(chunk, src, dst, n, size, s_sem, r_sem, target):
        def one(i, c):
            j = block_of(i, chunk)
            there = j // 2 * 2 + core
            cols = pl.ds(n, size)
            pltpu.make_async_remote_copy(
                src_ref=src.at[j, :, cols],
                dst_ref=dst.at[there, :, cols],
                send_sem=s_sem,
                recv_sem=r_sem,
                device_id=(base + j % 2, target(j, chunk)),
                device_id_type=MESH,
            ).start()
            return c

        lax.fori_loop(0, others(chunk), one, 0)

    def wait(chunk, ref, n, size, sem):
        part = ref.at[pl.ds(0, others(chunk)), :, pl.ds(n, size)]
        pltpu.make_async_copy(part, part, sem).wait()

    rows_c = 2 * blocks * 16
    hit, quarter = gather_mask(2, rows_c)
    picks = [ones(hit & (quarter == q)) for q in range(4)]
    for n in range(0, NT, FT):
        total = None
        for q in range(4):
            if q * NT + n < width:
                part = dot(picks[q], xs[:, q * NT + n : q * NT + n + FT])
                total = part if total is None else total + part
        snd_c[:, :, n : n + FT] = total.astype(jnp.bfloat16).reshape(2 * blocks, 16, FT)
    rcv_c[core] = snd_c[core]

    pl.semaphore_wait(barrier, others(2))
    send(2, snd_c, rcv_c, 0, NT, sem_ds.at[2], sem_dr.at[2], ahead)
    for chunk in range(2):
        hit, _ = gather_mask(chunk, blocks * 16)
        pick = ones(hit)
        for n, size in tiles:
            z = dot(pick, xs[:, n : n + size]).astype(jnp.bfloat16)
            snd[chunk, :, :, n : n + size] = z.reshape(blocks, 16, size)
        if chunk == 0:
            rcv[0, core] = snd[0, core]
        send(chunk, snd.at[chunk], rcv.at[chunk], 0, width, sem_ds.at[chunk], sem_dr.at[chunk], ahead)

    rows_z = zc.shape[0]

    def unstack(q):
        r = lax.broadcasted_iota(jnp.int32, (rows_z, rows_c), 0)
        s = lax.broadcasted_iota(jnp.int32, (rows_z, rows_c), 1)
        return ones(s == (r // 4) * 16 + q * 4 + r % 4)

    def stack(q):
        s = lax.broadcasted_iota(jnp.int32, (rows_c, rows_z), 0)
        r = lax.broadcasted_iota(jnp.int32, (rows_c, rows_z), 1)
        return ones((r == (s // 16) * 4 + s % 4) & ((s % 16) // 4 == q))

    for chunk in (2, 0, 1):
        first = chunk == 2
        if chunk == 2:
            wait(2, rcv_c, 0, NT, sem_dr.at[2])
            rem = rcv_c[...].reshape(rows_c, NT)
            for q, (n, size) in enumerate(tiles):
                zc[:, n : n + size] = dot(unstack(q), rem[:, :size]).astype(jnp.bfloat16)
            rows = rows_z
            load = lambda: zc[...]
        else:
            wait(chunk, rcv.at[chunk], 0, width, sem_dr.at[chunk])
            rows = blocks * 16
            load = lambda chunk=chunk: rcv[chunk].reshape(blocks * 16, width)

        def step(s):
            if first:
                for copy in gu_copies(s):
                    copy.wait()
            r = dot(load(), gu[s])
            a, b = r[:, :FT], r[:, FT:]
            h[0:rows, pl.ds(pl.multiple_of(s * FT, FT), FT)] = (
                a * jax.nn.sigmoid(a) * b
            ).astype(jnp.bfloat16)

        def body(i, c):
            for u in range(UNROLL):
                step(i * UNROLL + u)
            return c

        lax.fori_loop(0, steps // UNROLL, body, 0)
        for s in range(steps // UNROLL * UNROLL, steps):
            step(s)

        if chunk == 2:
            wait(2, snd_c, 0, NT, sem_ds.at[2])
        else:
            wait(chunk, snd.at[chunk], 0, width, sem_ds.at[chunk])
        for t, (n, size) in enumerate(tiles):
            if first:
                dn_copy(t).wait()
            out = dot(h[0:rows], dn[:, n : n + size]).astype(jnp.bfloat16)
            if chunk == 2:
                zc[:, n : n + size] = out
                continue
            snd[chunk, :, :, n : n + size] = out.reshape(blocks, 16, size)
            if chunk == 0:
                ret[0, core, :, n : n + size] = snd[0, core, :, n : n + size]
            send(chunk, snd.at[chunk], ret.at[chunk], n, size, sem_cs.at[chunk], sem_cr.at[chunk, t], behind)
        if chunk == 2:
            for n in range(0, NT, FT):
                total = None
                for q in range(4):
                    if q * NT + n < width:
                        part = dot(stack(q), zc[:, q * NT + n : q * NT + n + FT])
                        total = part if total is None else total + part
                snd_c[:, :, n : n + FT] = total.astype(jnp.bfloat16).reshape(2 * blocks, 16, FT)
            ret_c[core] = snd_c[core]
            send(2, snd_c, ret_c, 0, NT, sem_cs.at[2], sem_cr.at[2, 0], behind)

    def weights(chunk, rows):
        row = lax.broadcasted_iota(jnp.int32, (tokens, rows), 1)
        code, quarter = row_code(row, chunk)
        w = jnp.where(code == down0, gates[:, 0:1], 0.0) + jnp.where(code == down1, gates[:, 1:2], 0.0)
        if chunk == 2:
            w = jnp.where(row % 4 < rest, w, 0.0)
        return w, quarter

    w0 = weights(0, blocks * 16)[0].astype(jnp.bfloat16)
    w1 = weights(1, blocks * 16)[0].astype(jnp.bfloat16)
    w2, quarter = weights(2, rows_c)
    wait(2, ret_c, 0, NT, sem_cr.at[2, 0])
    for t, (n, size) in enumerate(tiles):
        wait(0, ret.at[0], n, size, sem_cr.at[0, t])
        total = dot(
            jnp.where(quarter == t, w2, 0.0).astype(jnp.bfloat16),
            ret_c[:, :, :size].reshape(rows_c, size),
        )
        total += dot(w0, ret[0, :, :, n : n + size].reshape(blocks * 16, size))
        wait(1, ret.at[1], n, size, sem_cr.at[1, t])
        total += dot(w1, ret[1, :, :, n : n + size].reshape(blocks * 16, size))
        xs[:, n : n + size] = total.astype(jnp.bfloat16)
        pltpu.make_async_copy(
            xs.at[:, pl.ds(n, size)], y_hbm.at[0, 0, :, pl.ds(n, size)], sem_y.at[t]
        ).start()
    for chunk in range(2):
        wait(chunk, snd.at[chunk], 0, width, sem_cs.at[chunk])
    wait(2, snd_c, 0, NT, sem_cs.at[2])
    for t, (n, size) in enumerate(tiles):
        pltpu.make_async_copy(
            xs.at[:, pl.ds(n, size)], y_hbm.at[0, 0, :, pl.ds(n, size)], sem_y.at[t]
        ).wait()


def layer(side, slots, x, expert, slot, gate, wg, wu, wd):
    tokens, width = x.shape[2:]
    hidden = wg.shape[2]
    blocks = side * side
    tiles = -(-width // NT)
    vmem, hbm = pl.BlockSpec(memory_space=pltpu.VMEM), pl.BlockSpec(memory_space=pl.ANY)
    bf16, sem = jnp.bfloat16, pltpu.SemaphoreType.DMA
    return pl.pallas_call(
        functools.partial(kernel, side, slots),
        out_shape=jax.ShapeDtypeStruct(x.shape, bf16),
        in_specs=[hbm, vmem, vmem, vmem, hbm, hbm, hbm],
        out_specs=hbm,
        scratch_shapes=[
            pltpu.VMEM((tokens, width), bf16),
            pltpu.VMEM((hidden // FT, width, 2 * FT), bf16),
            pltpu.VMEM((hidden, width), bf16),
            pltpu.VMEM((blocks * 16, hidden), bf16),
            pltpu.VMEM((2 * blocks * 4, width), bf16),
            pltpu.VMEM((2, blocks, 16, width), bf16),
            pltpu.VMEM((2 * blocks, 16, NT), bf16),
            pltpu.VMEM((2, blocks, 16, width), bf16),
            pltpu.VMEM((2 * blocks, 16, NT), bf16),
            pltpu.VMEM((2, blocks, 16, width), bf16),
            pltpu.VMEM((2 * blocks, 16, NT), bf16),
            sem(()),
            sem((hidden // FT, 2)),
            sem((tiles,)),
            sem((3,)),
            sem((3,)),
            sem((3,)),
            sem((3, tiles)),
            sem((tiles,)),
        ],
        compiler_params=pltpu.CompilerParams(
            collective_id=0, has_side_effects=True, vmem_limit_bytes=67043328
        ),
        name="moe_layer",
    )(x, expert, slot, gate, wg, wu, wd)


def solution(mesh):
    members = mesh.shape["ep"]
    side = round(members**0.5)

    def step(x, expert, slot, gate, w_gate, w_up, w_down):
        experts, (tokens, top) = w_gate.shape[0], expert.shape[2:]
        slots = 5 * tokens * top // (4 * experts)
        act, w = P("dp", "ep"), P("ep")
        return jax.shard_map(
            functools.partial(layer, side, slots),
            mesh=mesh,
            in_specs=(act, act, act, act, w, w, w),
            out_specs=act,
            check_vma=False,
        )(x, expert, slot, gate, w_gate, w_up, w_down)

    return step
```

```python
import functools

import jax
import jax.numpy as jnp
from jax import lax
from jax.experimental import pallas as pl
from jax.experimental.pallas import tpu as pltpu
from jax.sharding import PartitionSpec as P

MESH = pl.DeviceIdType.MESH
FT = 256
NT = 512
ROWS = 16
UNROLL = 3
PARTS = (
    ((0, 0), (2, 0), (0, 2), (2, 2)),
    ((1, 1), (3, 3), (1, 3), (3, 1)),
    ((2, 1), (0, 3), (2, 3), (0, 1)),
    ((1, 2), (3, 0), (3, 2), (1, 0)),
)
CHUNKS = ((), (0,), (1, 2), (3,))


def dot(a, b):
    return jnp.dot(a, b, preferred_element_type=jnp.float32)


def kernel(
    side, slots,
    x_hbm, expert_ref, slot_ref, gate_ref, wg, wu, wd, y_hbm,
    xs, wts, gu, dn, h, zc, snd, snd_c, rcv, rcv_c, ret, ret_c,
    sem_x, sem_g, sem_d, sem_ds, sem_dr, sem_cs, sem_cr, sem_y,
):
    members = side * side
    tokens, width = xs.shape
    hidden = h.shape[1]
    steps = hidden // FT
    rest = slots - ROWS
    dp, ep = lax.axis_index("dp"), lax.axis_index("ep")
    core = lax.rem(dp, 2)
    base = dp - core
    px, py = ep // side, lax.rem(ep, side)
    tiles = [(n, min(NT, width - n)) for n in range(0, width, NT)]
    blocks = 2 * members
    size_p = blocks // len(PARTS)

    def place(i):
        q, b = i // size_p, (i % size_p) // 2
        return 2 * (b // 2) + q % 2, 2 * (b % 2) + (q + q // 2) % 2

    def ahead(i):
        dx, dy = place(i)
        return ((px + dx) % side) * side + (py + dy) % side

    def behind(i):
        dx, dy = place(i)
        return ((px + side - dx) % side) * side + (py + side - dy) % side

    def remote(parts):
        parts = parts or range(len(PARTS))
        return len(parts) * size_p - (0 in parts)

    def sends(parts):
        for q in parts or range(len(PARTS)):
            for dx, dy in PARTS[q]:
                i = q * size_p + 2 * (dx // 2 * 2 + dy // 2)
                if dx == dy == 0:
                    yield 1 - core
                else:
                    yield i
                    yield i + 1

    copy_x = pltpu.make_async_copy(x_hbm.at[0, 0], xs, sem_x)
    copy_x.start()

    barrier = pltpu.get_barrier_semaphore()

    def greet(i, c):
        j = (i + 1) // 2 * 2 + (i + 1 + core) % 2
        pl.semaphore_signal(
            barrier, inc=1, device_id=(base + j % 2, ahead(j)), device_id_type=MESH
        )
        return c

    lax.fori_loop(0, blocks - 1, greet, 0)

    def gu_copies(s):
        cols = pl.ds(pl.multiple_of(s * FT, FT), FT)
        return (
            pltpu.make_async_copy(wg.at[core, :, cols], gu.at[s, :, pl.ds(0, FT)], sem_g.at[s, 0]),
            pltpu.make_async_copy(wu.at[core, :, cols], gu.at[s, :, pl.ds(FT, FT)], sem_g.at[s, 1]),
        )

    def dn_copy(t):
        n, size = tiles[t]
        return pltpu.make_async_copy(wd.at[core, :, pl.ds(n, size)], dn.at[:, pl.ds(n, size)], sem_d.at[t])

    copy_x.wait()

    def start_gu(s, c):
        for copy in gu_copies(s):
            copy.start()
        return c

    lax.fori_loop(0, steps, start_gu, 0)
    for t in range(len(tiles)):
        dn_copy(t).start()

    slot, expert = slot_ref[0, 0], expert_ref[0, 0]
    code = jnp.where(slot < slots, expert * slots + slot, -1)
    across0, across1 = code[0:1], code[1:2]

    def upright(v):
        return jnp.transpose(jnp.broadcast_to(v, (128, tokens)))[:, 0:1]

    def row_code(row):
        i = row // 16
        return (2 * ahead(i) + i % 2) * slots + row % 16

    def rest_code(row):
        i, j = row // 16, row % 16
        code = (2 * ahead(i) + i % 2) * slots + ROWS + j % 4
        return jnp.where(j % 4 < rest, code, -2), j // 4

    def ones(mask):
        return jnp.where(mask, 1.0, 0.0).astype(jnp.bfloat16)

    def send(parts, src, dst, n, size, s_sem, r_sem, target):
        for j in sends(parts):
            there = core if isinstance(j, jax.Array) else j // 2 * 2 + core
            cols = pl.ds(n, size)
            pltpu.make_async_remote_copy(
                src_ref=src.at[j, :, cols],
                dst_ref=dst.at[there, :, cols],
                send_sem=s_sem,
                recv_sem=r_sem,
                device_id=(base + j % 2, target(j)),
                device_id_type=MESH,
            ).start()

    def wait(parts, ref, n, size, sem):
        part = ref.at[pl.ds(0, remote(parts)), :, pl.ds(n, size)]
        pltpu.make_async_copy(part, part, sem).wait()

    rows_c = blocks * 16
    rows_p = size_p * 16
    code, quarter = rest_code(lax.broadcasted_iota(jnp.int32, (rows_c, tokens), 0))
    hit = (code == across0) | (code == across1)
    picks = [ones(hit & (quarter == q)) for q in range(4)]
    for n in range(0, NT, FT):
        total = None
        for q in range(4):
            if q * NT + n < width:
                part = dot(picks[q], xs[:, q * NT + n : q * NT + n + FT])
                total = part if total is None else total + part
        snd_c[:, :, n : n + FT] = total.astype(jnp.bfloat16).reshape(blocks, 16, FT)
    rcv_c[core] = snd_c[core]

    pl.semaphore_wait(barrier, blocks - 1)
    send((), snd_c, rcv_c, 0, NT, sem_ds.at[0], sem_dr.at[0], ahead)
    for c, parts in enumerate(CHUNKS):
        for q in parts:
            i = q * size_p
            code = row_code(lax.broadcasted_iota(jnp.int32, (rows_p, tokens), 0) + q * rows_p)
            pick = ones((code == across0) | (code == across1))
            for n, size in tiles:
                z = dot(pick, xs[:, n : n + size]).astype(jnp.bfloat16)
                snd[i : i + size_p, :, n : n + size] = z.reshape(size_p, 16, size)
            if q == 0:
                rcv[core] = snd[core]
            send((q,), snd, rcv, 0, width, sem_ds.at[c], sem_dr.at[c], ahead)

    down0, down1 = upright(across0), upright(across1)
    gates = gate_ref[0, 0].astype(jnp.bfloat16).astype(jnp.float32)
    gate0, gate1 = upright(gates[0:1]), upright(gates[1:2])
    row = lax.broadcasted_iota(jnp.int32, (tokens, rows_c), 1)
    for i, code in enumerate((row_code(row), rest_code(row)[0])):
        w = jnp.where(code == down0, gate0, 0.0) + jnp.where(code == down1, gate1, 0.0)
        wts[:, i * rows_c : (i + 1) * rows_c] = w.astype(jnp.bfloat16)

    rows_z = zc.shape[0]

    def unstack(q):
        r = lax.broadcasted_iota(jnp.int32, (rows_z, rows_c), 0)
        s = lax.broadcasted_iota(jnp.int32, (rows_z, rows_c), 1)
        return ones(s == (r // 4) * 16 + q * 4 + r % 4)

    def stack(q):
        s = lax.broadcasted_iota(jnp.int32, (rows_c, rows_z), 0)
        r = lax.broadcasted_iota(jnp.int32, (rows_c, rows_z), 1)
        return ones((r == (s // 16) * 4 + s % 4) & ((s % 16) // 4 == q))

    for c, parts in enumerate(CHUNKS):
        first = c == 0
        if parts:
            wait(parts, rcv, 0, width, sem_dr.at[c])
            rows, i = len(parts) * rows_p, parts[0] * size_p
            load = lambda i=i, rows=rows: rcv[i : i + rows // 16].reshape(rows, width)
        else:
            wait((), rcv_c, 0, NT, sem_dr.at[c])
            rem = rcv_c[...].reshape(rows_c, NT)
            for q, (n, size) in enumerate(tiles):
                zc[:, n : n + size] = dot(unstack(q), rem[:, :size]).astype(jnp.bfloat16)
            rows = rows_z
            load = lambda: zc[...]

        def step(s):
            if first:
                for copy in gu_copies(s):
                    copy.wait()
            r = dot(load(), gu[s])
            a, b = r[:, :FT], r[:, FT:]
            h[0:rows, pl.ds(pl.multiple_of(s * FT, FT), FT)] = (
                a * jax.nn.sigmoid(a) * b
            ).astype(jnp.bfloat16)

        def body(i, c):
            for u in range(UNROLL):
                step(i * UNROLL + u)
            return c

        lax.fori_loop(0, steps // UNROLL, body, 0)
        for s in range(steps // UNROLL * UNROLL, steps):
            step(s)

        if parts:
            wait(parts, snd, 0, width, sem_ds.at[c])
        else:
            wait((), snd_c, 0, NT, sem_ds.at[c])
        for t, (n, size) in enumerate(tiles):
            if first:
                dn_copy(t).wait()
            out = dot(h[0:rows], dn[:, n : n + size]).astype(jnp.bfloat16)
            if not parts:
                zc[:, n : n + size] = out
                continue
            snd[i : i + rows // 16, :, n : n + size] = out.reshape(rows // 16, 16, size)
            if 0 in parts:
                ret[core, :, n : n + size] = snd[core, :, n : n + size]
            send(parts, snd, ret, n, size, sem_cs.at[c], sem_cr.at[c, t], behind)
        if not parts:
            for n in range(0, NT, FT):
                total = None
                for q in range(4):
                    if q * NT + n < width:
                        part = dot(stack(q), zc[:, q * NT + n : q * NT + n + FT])
                        total = part if total is None else total + part
                snd_c[:, :, n : n + FT] = total.astype(jnp.bfloat16).reshape(blocks, 16, FT)
            ret_c[core] = snd_c[core]
            send((), snd_c, ret_c, 0, NT, sem_cs.at[c], sem_cr.at[c, 0], behind)

    _, quarter = rest_code(lax.broadcasted_iota(jnp.int32, (tokens, rows_c), 1))
    early = rows_c - len(CHUNKS[-1]) * rows_p
    for t, (n, size) in enumerate(tiles):
        for c, parts in enumerate(CHUNKS[:-1]):
            if parts:
                wait(parts, ret, n, size, sem_cr.at[c, t])
            elif t == 0:
                wait((), ret_c, 0, NT, sem_cr.at[c, 0])
        w = wts[:, rows_c:].astype(jnp.float32)
        w = jnp.where(quarter == t, w, 0.0).astype(jnp.bfloat16)
        total = dot(w, ret_c[:, :, :size].reshape(rows_c, size))
        rows = ret[: early // 16, :, n : n + size].reshape(early, size)
        total += dot(wts[:, :early], rows)
        wait(CHUNKS[-1], ret, n, size, sem_cr.at[len(CHUNKS) - 1, t])
        rows = ret[early // 16 :, :, n : n + size].reshape(rows_c - early, size)
        total += dot(wts[:, early:rows_c], rows)
        xs[:, n : n + size] = total.astype(jnp.bfloat16)
        pltpu.make_async_copy(
            xs.at[:, pl.ds(n, size)], y_hbm.at[0, 0, :, pl.ds(n, size)], sem_y.at[t]
        ).start()
    for c, parts in enumerate(CHUNKS):
        if parts:
            wait(parts, snd, 0, width, sem_cs.at[c])
        else:
            wait((), snd_c, 0, NT, sem_cs.at[c])
    for t, (n, size) in enumerate(tiles):
        pltpu.make_async_copy(
            xs.at[:, pl.ds(n, size)], y_hbm.at[0, 0, :, pl.ds(n, size)], sem_y.at[t]
        ).wait()


def layer(side, slots, x, expert, slot, gate, wg, wu, wd):
    tokens, width = x.shape[2:]
    hidden = wg.shape[2]
    blocks = 2 * side * side
    tiles, chunks = -(-width // NT), len(CHUNKS)
    largest = max(map(len, CHUNKS)) * blocks // len(PARTS) * 16
    vmem, hbm = pl.BlockSpec(memory_space=pltpu.VMEM), pl.BlockSpec(memory_space=pl.ANY)
    bf16, sem = jnp.bfloat16, pltpu.SemaphoreType.DMA
    whole, quarters = pltpu.VMEM((blocks, 16, width), bf16), pltpu.VMEM((blocks, 16, NT), bf16)
    return pl.pallas_call(
        functools.partial(kernel, side, slots),
        out_shape=jax.ShapeDtypeStruct(x.shape, bf16),
        in_specs=[hbm, vmem, vmem, vmem, hbm, hbm, hbm],
        out_specs=hbm,
        scratch_shapes=[
            pltpu.VMEM((tokens, width), bf16),
            pltpu.VMEM((tokens, 2 * blocks * 16), bf16),
            pltpu.VMEM((hidden // FT, width, 2 * FT), bf16),
            pltpu.VMEM((hidden, width), bf16),
            pltpu.VMEM((largest, hidden), bf16),
            pltpu.VMEM((blocks * 4, width), bf16),
            whole,
            quarters,
            whole,
            quarters,
            whole,
            quarters,
            sem(()),
            sem((hidden // FT, 2)),
            sem((tiles,)),
            sem((chunks,)),
            sem((chunks,)),
            sem((chunks,)),
            sem((chunks, tiles)),
            sem((tiles,)),
        ],
        compiler_params=pltpu.CompilerParams(
            collective_id=0, has_side_effects=True, vmem_limit_bytes=67043328
        ),
        name="moe_layer",
    )(x, *(jnp.swapaxes(v, 2, 3) for v in (expert, slot, gate)), wg, wu, wd)


def solution(mesh):
    members = mesh.shape["ep"]
    side = round(members**0.5)

    def step(x, expert, slot, gate, w_gate, w_up, w_down):
        experts, (tokens, top) = w_gate.shape[0], expert.shape[2:]
        slots = 5 * tokens * top // (4 * experts)
        act, w = P("dp", "ep"), P("ep")
        return jax.shard_map(
            functools.partial(layer, side, slots),
            mesh=mesh,
            in_specs=(act, act, act, act, w, w, w),
            out_specs=act,
            check_vma=False,
        )(x, expert, slot, gate, w_gate, w_up, w_down)

    return step
```

```python
import functools

import jax
import jax.numpy as jnp
from jax import lax
from jax.experimental import pallas as pl
from jax.experimental.pallas import tpu as pltpu
from jax.sharding import PartitionSpec as P

MESH = pl.DeviceIdType.MESH
FT = 256
NT = 512
ROWS = 16
UNROLL = 6
PHASES = (
    ((0, 0), (2, 0), (0, 2), (1, 1), (3, 3), (1, 3), (3, 1), (2, 2)),
    ((2, 1), (0, 3), (2, 3), (0, 1), (1, 2), (3, 0), (3, 2), (1, 0)),
)


def dot(a, b):
    return jnp.dot(a, b, preferred_element_type=jnp.float32)


def kernel(
    side, slots,
    x_hbm, expert_ref, slot_ref, gate_ref, wg, wu, wd, y_hbm,
    xs, wts, gu, dn, h, zc, snd, snd_c, rcv, rcv_c, ret, ret_c,
    sem_x, sem_g, sem_d, sem_ds, sem_dr, sem_cs, sem_cr, sem_y,
):
    members = side * side
    tokens, width = xs.shape
    hidden = h.shape[1]
    steps = hidden // FT
    rest = slots - ROWS
    dp, ep = lax.axis_index("dp"), lax.axis_index("ep")
    core = lax.rem(dp, 2)
    base = dp - core
    px, py = ep // side, lax.rem(ep, side)
    tiles = [(n, min(NT, width - n)) for n in range(0, width, NT)]
    blocks = members

    def place(i, chunk):
        b = i // 2
        if chunk == 2:
            return b // side, b % side
        dx = b // 2
        return dx, 2 * (b % 2) + (dx + chunk) % 2

    def ahead(i, chunk):
        dx, dy = place(i, chunk)
        return ((px + dx) % side) * side + (py + dy) % side

    def behind(i, chunk):
        dx, dy = place(i, chunk)
        return ((px + side - dx) % side) * side + (py + side - dy) % side

    def others(chunk):
        return {0: blocks - 1, 1: blocks, 2: 2 * blocks - 1}[chunk]

    def sends(chunk):
        for dx, dy in PHASES[0] + PHASES[1] if chunk == 2 else PHASES[chunk]:
            b = dx * side + dy if chunk == 2 else 2 * dx + dy // 2
            if dx == dy == 0:
                yield 1 - core
            else:
                yield 2 * b
                yield 2 * b + 1

    copy_x = pltpu.make_async_copy(x_hbm.at[0, 0], xs, sem_x)
    copy_x.start()

    barrier = pltpu.get_barrier_semaphore()

    def greet(i, c):
        j = (i + 1) // 2 * 2 + (i + 1 + core) % 2
        pl.semaphore_signal(
            barrier, inc=1, device_id=(base + j % 2, ahead(j, 2)), device_id_type=MESH
        )
        return c

    lax.fori_loop(0, others(2), greet, 0)

    def gu_copies(s):
        cols = pl.ds(pl.multiple_of(s * FT, FT), FT)
        return (
            pltpu.make_async_copy(wg.at[core, :, cols], gu.at[s, :, pl.ds(0, FT)], sem_g.at[s, 0]),
            pltpu.make_async_copy(wu.at[core, :, cols], gu.at[s, :, pl.ds(FT, FT)], sem_g.at[s, 1]),
        )

    def dn_copy(t):
        n, size = tiles[t]
        return pltpu.make_async_copy(wd.at[core, :, pl.ds(n, size)], dn.at[:, pl.ds(n, size)], sem_d.at[t])

    copy_x.wait()

    def start_gu(s, c):
        for copy in gu_copies(s):
            copy.start()
        return c

    lax.fori_loop(0, steps, start_gu, 0)
    for t in range(len(tiles)):
        dn_copy(t).start()

    slot, expert = slot_ref[0, 0], expert_ref[0, 0]
    code = jnp.where(slot < slots, expert * slots + slot, -1)
    across0, across1 = code[0:1], code[1:2]

    def upright(v):
        return jnp.transpose(jnp.broadcast_to(v, (128, tokens)))[:, 0:1]

    def row_code(row, chunk):
        i, j = row // 16, row % 16
        if chunk == 2:
            return (2 * ahead(i, 2) + i % 2) * slots + ROWS + j % 4, j // 4
        return (2 * ahead(i, chunk) + i % 2) * slots + j, None

    def gather_mask(chunk, rows):
        row = lax.broadcasted_iota(jnp.int32, (rows, tokens), 0)
        code, quarter = row_code(row, chunk)
        hit = (code == across0) | (code == across1)
        if chunk == 2:
            hit = hit & (row % 4 < rest)
        return hit, quarter

    def ones(mask):
        return jnp.where(mask, 1.0, 0.0).astype(jnp.bfloat16)

    def send(chunk, src, dst, n, size, s_sem, r_sem, target):
        for j in sends(chunk):
            there = core if isinstance(j, jax.Array) else j // 2 * 2 + core
            cols = pl.ds(n, size)
            pltpu.make_async_remote_copy(
                src_ref=src.at[j, :, cols],
                dst_ref=dst.at[there, :, cols],
                send_sem=s_sem,
                recv_sem=r_sem,
                device_id=(base + j % 2, target(j, chunk)),
                device_id_type=MESH,
            ).start()

    def wait(chunk, ref, n, size, sem):
        part = ref.at[pl.ds(0, others(chunk)), :, pl.ds(n, size)]
        pltpu.make_async_copy(part, part, sem).wait()

    rows_c = 2 * blocks * 16
    hit, quarter = gather_mask(2, rows_c)
    picks = [ones(hit & (quarter == q)) for q in range(4)]
    for n in range(0, NT, FT):
        total = None
        for q in range(4):
            if q * NT + n < width:
                part = dot(picks[q], xs[:, q * NT + n : q * NT + n + FT])
                total = part if total is None else total + part
        snd_c[:, :, n : n + FT] = total.astype(jnp.bfloat16).reshape(2 * blocks, 16, FT)
    rcv_c[core] = snd_c[core]

    pl.semaphore_wait(barrier, others(2))
    send(2, snd_c, rcv_c, 0, NT, sem_ds.at[2], sem_dr.at[2], ahead)
    for chunk in range(2):
        hit, _ = gather_mask(chunk, blocks * 16)
        pick = ones(hit)
        for n, size in tiles:
            z = dot(pick, xs[:, n : n + size]).astype(jnp.bfloat16)
            snd[chunk, :, :, n : n + size] = z.reshape(blocks, 16, size)
        if chunk == 0:
            rcv[0, core] = snd[0, core]
        send(chunk, snd.at[chunk], rcv.at[chunk], 0, width, sem_ds.at[chunk], sem_dr.at[chunk], ahead)

    down0, down1 = upright(across0), upright(across1)
    gates = gate_ref[0, 0].astype(jnp.bfloat16).astype(jnp.float32)
    gate0, gate1 = upright(gates[0:1]), upright(gates[1:2])
    at = 0
    for chunk, rows in ((0, blocks * 16), (1, blocks * 16), (2, rows_c)):
        row = lax.broadcasted_iota(jnp.int32, (tokens, rows), 1)
        code, _ = row_code(row, chunk)
        w = jnp.where(code == down0, gate0, 0.0) + jnp.where(code == down1, gate1, 0.0)
        if chunk == 2:
            w = jnp.where(row % 4 < rest, w, 0.0)
        wts[:, at : at + rows] = w.astype(jnp.bfloat16)
        at += rows

    rows_z = zc.shape[0]

    def unstack(q):
        r = lax.broadcasted_iota(jnp.int32, (rows_z, rows_c), 0)
        s = lax.broadcasted_iota(jnp.int32, (rows_z, rows_c), 1)
        return ones(s == (r // 4) * 16 + q * 4 + r % 4)

    def stack(q):
        s = lax.broadcasted_iota(jnp.int32, (rows_c, rows_z), 0)
        r = lax.broadcasted_iota(jnp.int32, (rows_c, rows_z), 1)
        return ones((r == (s // 16) * 4 + s % 4) & ((s % 16) // 4 == q))

    for chunk in (2, 0, 1):
        first = chunk == 2
        if chunk == 2:
            wait(2, rcv_c, 0, NT, sem_dr.at[2])
            rem = rcv_c[...].reshape(rows_c, NT)
            for q, (n, size) in enumerate(tiles):
                zc[:, n : n + size] = dot(unstack(q), rem[:, :size]).astype(jnp.bfloat16)
            rows = rows_z
            load = lambda: zc[...]
        else:
            wait(chunk, rcv.at[chunk], 0, width, sem_dr.at[chunk])
            rows = blocks * 16
            load = lambda chunk=chunk: rcv[chunk].reshape(blocks * 16, width)

        def step(s):
            if first:
                for copy in gu_copies(s):
                    copy.wait()
            r = dot(load(), gu[s])
            a, b = r[:, :FT], r[:, FT:]
            h[0:rows, pl.ds(pl.multiple_of(s * FT, FT), FT)] = (
                a * jax.nn.sigmoid(a) * b
            ).astype(jnp.bfloat16)

        def body(i, c):
            for u in range(UNROLL):
                step(i * UNROLL + u)
            return c

        lax.fori_loop(0, steps // UNROLL, body, 0)
        for s in range(steps // UNROLL * UNROLL, steps):
            step(s)

        if chunk == 2:
            wait(2, snd_c, 0, NT, sem_ds.at[2])
        else:
            wait(chunk, snd.at[chunk], 0, width, sem_ds.at[chunk])
        for t, (n, size) in enumerate(tiles):
            if first:
                dn_copy(t).wait()
            out = dot(h[0:rows], dn[:, n : n + size]).astype(jnp.bfloat16)
            if chunk == 2:
                zc[:, n : n + size] = out
                continue
            snd[chunk, :, :, n : n + size] = out.reshape(blocks, 16, size)
            if chunk == 0:
                ret[0, core, :, n : n + size] = snd[0, core, :, n : n + size]
            send(chunk, snd.at[chunk], ret.at[chunk], n, size, sem_cs.at[chunk], sem_cr.at[chunk, t], behind)
        if chunk == 2:
            for n in range(0, NT, FT):
                total = None
                for q in range(4):
                    if q * NT + n < width:
                        part = dot(stack(q), zc[:, q * NT + n : q * NT + n + FT])
                        total = part if total is None else total + part
                snd_c[:, :, n : n + FT] = total.astype(jnp.bfloat16).reshape(2 * blocks, 16, FT)
            ret_c[core] = snd_c[core]
            send(2, snd_c, ret_c, 0, NT, sem_cs.at[2], sem_cr.at[2, 0], behind)

    w0 = wts[:, 0 : blocks * 16]
    w1 = wts[:, blocks * 16 : 2 * blocks * 16]
    w2 = wts[:, 2 * blocks * 16 :].astype(jnp.float32)
    _, quarter = row_code(lax.broadcasted_iota(jnp.int32, (tokens, rows_c), 1), 2)
    wait(2, ret_c, 0, NT, sem_cr.at[2, 0])
    for t, (n, size) in enumerate(tiles):
        wait(0, ret.at[0], n, size, sem_cr.at[0, t])
        total = dot(
            jnp.where(quarter == t, w2, 0.0).astype(jnp.bfloat16),
            ret_c[:, :, :size].reshape(rows_c, size),
        )
        total += dot(w0, ret[0, :, :, n : n + size].reshape(blocks * 16, size))
        wait(1, ret.at[1], n, size, sem_cr.at[1, t])
        total += dot(w1, ret[1, :, :, n : n + size].reshape(blocks * 16, size))
        xs[:, n : n + size] = total.astype(jnp.bfloat16)
        pltpu.make_async_copy(
            xs.at[:, pl.ds(n, size)], y_hbm.at[0, 0, :, pl.ds(n, size)], sem_y.at[t]
        ).start()
    for chunk in range(2):
        wait(chunk, snd.at[chunk], 0, width, sem_cs.at[chunk])
    wait(2, snd_c, 0, NT, sem_cs.at[2])
    for t, (n, size) in enumerate(tiles):
        pltpu.make_async_copy(
            xs.at[:, pl.ds(n, size)], y_hbm.at[0, 0, :, pl.ds(n, size)], sem_y.at[t]
        ).wait()


def layer(side, slots, x, expert, slot, gate, wg, wu, wd):
    tokens, width = x.shape[2:]
    hidden = wg.shape[2]
    blocks = side * side
    tiles = -(-width // NT)
    vmem, hbm = pl.BlockSpec(memory_space=pltpu.VMEM), pl.BlockSpec(memory_space=pl.ANY)
    bf16, sem = jnp.bfloat16, pltpu.SemaphoreType.DMA
    return pl.pallas_call(
        functools.partial(kernel, side, slots),
        out_shape=jax.ShapeDtypeStruct(x.shape, bf16),
        in_specs=[hbm, vmem, vmem, vmem, hbm, hbm, hbm],
        out_specs=hbm,
        scratch_shapes=[
            pltpu.VMEM((tokens, width), bf16),
            pltpu.VMEM((tokens, 4 * blocks * 16), bf16),
            pltpu.VMEM((hidden // FT, width, 2 * FT), bf16),
            pltpu.VMEM((hidden, width), bf16),
            pltpu.VMEM((blocks * 16, hidden), bf16),
            pltpu.VMEM((2 * blocks * 4, width), bf16),
            pltpu.VMEM((2, blocks, 16, width), bf16),
            pltpu.VMEM((2 * blocks, 16, NT), bf16),
            pltpu.VMEM((2, blocks, 16, width), bf16),
            pltpu.VMEM((2 * blocks, 16, NT), bf16),
            pltpu.VMEM((2, blocks, 16, width), bf16),
            pltpu.VMEM((2 * blocks, 16, NT), bf16),
            sem(()),
            sem((hidden // FT, 2)),
            sem((tiles,)),
            sem((3,)),
            sem((3,)),
            sem((3,)),
            sem((3, tiles)),
            sem((tiles,)),
        ],
        compiler_params=pltpu.CompilerParams(
            collective_id=0, has_side_effects=True, vmem_limit_bytes=67043328
        ),
        name="moe_layer",
    )(x, *(jnp.swapaxes(v, 2, 3) for v in (expert, slot, gate)), wg, wu, wd)


def solution(mesh):
    members = mesh.shape["ep"]
    side = round(members**0.5)

    def step(x, expert, slot, gate, w_gate, w_up, w_down):
        experts, (tokens, top) = w_gate.shape[0], expert.shape[2:]
        slots = 5 * tokens * top // (4 * experts)
        act, w = P("dp", "ep"), P("ep")
        return jax.shard_map(
            functools.partial(layer, side, slots),
            mesh=mesh,
            in_specs=(act, act, act, act, w, w, w),
            out_specs=act,
            check_vma=False,
        )(x, expert, slot, gate, w_gate, w_up, w_down)

    return step
```
